128 devices in a mesh: rows: 32 (over y, x, core), rhs: 4 (over z).
Axes of the slice: x: 4, y: 4, z: 4, core: 2. Of those that a mesh axis runs over, the one named last changes fastest.
Arguments:
- band_blocks: float32 [256, 256, 1280], P('rows'), may hold values from -12 to 12
- precond_blocks: float32 [256, 256, 256], P('rows'), may hold values from -2 to 2
- right_side: float32 [65536, 2048], P('rows', 'rhs'), may hold values from -80 to 80
Outputs:
- solution: float32 [65536, 2048], P('rows', 'rhs')
- scaled_residual: float32 [65536, 2048], P('rows', 'rhs')
- rms_history: float32 [3, 2048], P(None, 'rhs')
- overall_rms: float32 [], replicated
The draws below stay inside these ranges and needn't reach their ends.
All inputs are finite; a program needn't handle non-finite values.
Results may differ from the reference program's by a relative error of at most 0.0003.
Values sent between devices are 32-bit elements; how exact they have to be, the bound alone decides.
A program may use at most 128 MiB of HBM per device.

```python
import math
import jax
import jax.numpy as jnp
from jax import lax

B = 256
ITERS = 2
NBLOCKS = 256
N = 65536
NRHS = 2048


def band_parts(key):
    base = jax.random.fold_in(key, 1234)
    key_scale, key_inner, key_outer = jax.random.split(base, 3)
    scales = jnp.exp(jax.random.uniform(key_scale, (NBLOCKS,), jnp.float32) * math.log(10.0))
    inner = jax.random.normal(key_inner, (NBLOCKS, B, B), jnp.float32) * (0.15 / math.sqrt(B))
    outer = jax.random.normal(key_outer, (NBLOCKS, B, 4 * B), jnp.float32) * (0.15 / math.sqrt(B))
    return (scales, inner, outer)


def draw_band_blocks(key, part):
    scales, inner, outer = band_parts(key)
    identity = jnp.eye(B, dtype=jnp.float32)
    center = scales[:, None, None] * (identity[None, :, :] + inner)
    pieces = []
    for number, offset in enumerate([-2, -1, 1, 2]):
        beside = jnp.roll(scales, -offset)
        pieces.append(outer[:, :, number * B:(number + 1) * B] * jnp.sqrt(scales * beside)[:, None, None])
    return jnp.concatenate([pieces[0], pieces[1], center, pieces[2], pieces[3]], axis=2)


def draw_precond_blocks(key, part):
    scales, inner, outer = band_parts(key)
    identity = jnp.eye(B, dtype=jnp.float32)
    square = jnp.einsum('jab,jbc->jac', inner, inner, precision=lax.Precision.HIGHEST)
    return (identity[None, :, :] - inner + square) / scales[:, None, None]


def draw_right_side(key, part):
    base = jax.random.fold_in(key, 77)
    key_value, key_column = jax.random.split(base, 2)
    row_frac = jnp.arange(N, dtype=jnp.float32) / N
    row_scale = jnp.exp(row_frac * math.log(10.0)) / math.sqrt(10.0)
    column_frac = jnp.arange(NRHS, dtype=jnp.float32) / NRHS
    column_scale = jnp.exp(column_frac * math.log(3.0)) * (1.0 + jax.random.uniform(key_column, (NRHS,), jnp.float32))
    values = jnp.clip(jax.random.normal(key_value, (N, NRHS), jnp.float32), -4.0, 4.0)
    return values * row_scale[:, None] * column_scale[None, :]


def setup_inputs(seed: int = 0) -> dict:
    seeds = jax.random.split(jax.random.key(seed), 4)
    return {
        "band_blocks": draw_band_blocks(jax.random.fold_in(seeds[3], 71), 0),
        "precond_blocks": draw_precond_blocks(jax.random.fold_in(seeds[3], 71), 0),
        "right_side": draw_right_side(jax.random.fold_in(seeds[3], 71), 0),
    }


def band_times(band_blocks, operand):
    padded = jnp.pad(operand, ((2 * B, 2 * B), (0, 0)))
    indices = jnp.arange(NBLOCKS, dtype=jnp.int32)

    def one_block(pair):
        block, index = pair
        window = lax.dynamic_slice_in_dim(padded, (index * B).astype(jnp.int32), 5 * B, 0)
        return jnp.dot(block, window, precision=lax.Precision.HIGHEST, preferred_element_type=jnp.float32)
    return lax.map(one_block, (band_blocks, indices)).reshape(operand.shape[0], operand.shape[1])

def precondition(precond_blocks, operand):
    shaped = operand.reshape(NBLOCKS, B, operand.shape[1])
    return jnp.einsum('jab,jbc->jac', precond_blocks, shaped, precision=lax.Precision.HIGHEST).reshape(operand.shape)

def reference(band_blocks, precond_blocks, right_side):
    solution = precondition(precond_blocks, right_side)
    sums = []
    residual = right_side
    for sweep in range(ITERS + 1):
        residual = right_side - band_times(band_blocks, solution)
        sums.append(lax.optimization_barrier(jnp.sum(residual * residual, axis=0)))
        if sweep < ITERS:
            solution = solution + precondition(precond_blocks, residual)
    stacked = jnp.stack(sums)
    history = jnp.sqrt(stacked / N + 1e-06)
    scaled_residual = residual / history[ITERS][None, :]
    overall_rms = jnp.sqrt(jnp.sum(stacked[ITERS]) / (N * NRHS) + 1e-06)
    return (solution, scaled_residual, history, overall_rms)
```

```python
import functools

import jax
import jax.numpy as jnp
from jax import lax
from jax.experimental import pallas as pl
from jax.experimental.pallas import tpu as pltpu
from jax.sharding import PartitionSpec as P

MESH = pl.DeviceIdType.MESH
F32, BF16 = jnp.float32, jnp.bfloat16
SWEEPS = 3
T = 256
LINE = 8


def split(value):
    high = value.astype(BF16)
    return high, (value - high.astype(F32)).astype(BF16)


def kernel(
    rows_n, rhs_n, blocks,
    band, precond, rhs,
    x, r, history, overall,
    a32, m32, ahi, alo, mhi, mlo, rhi, rlo, dhi, dlo, dsend, halo, hhi, hlo, part, msg, p1, mid, p2, zmsg, zbuf,
    a_sem, m_sem, b_sem, send_sem, recv_sem, p1_send, p1_recv, p2_send, p2_recv, z_send, z_recv,
):
    me = lax.axis_index("rows")
    z = lax.axis_index("rhs")
    lines = rows_n // LINE
    line, spot = me // LINE, me % LINE
    has = (me > 0, me < rows_n - 1)
    beside = (me - 1, me + 1)
    far = ((spot == 0) & has[0], (spot == LINE - 1) & has[1])
    chunks = rhs.shape[1] // T
    edge = (0, 1, blocks - 1, blocks - 2)
    inner = tuple(range(2, blocks // 2)), tuple(range(blocks - 3, blocks // 2 - 1, -1))
    inner_flat = tuple(j for pair in zip(*inner) for j in pair)

    def rows_of(j):
        return slice(j * T, (j + 1) * T)

    def cols_of(c):
        if isinstance(c, int):
            return slice(c * T, (c + 1) * T)
        return pl.ds(pl.multiple_of(c * T, T), T)

    def m_copy(j):
        return pltpu.make_async_copy(precond.at[j], m32.at[j], m_sem.at[j])

    def b_copy(j, c):
        return pltpu.make_async_copy(
            rhs.at[rows_of(j), cols_of(c)], r.at[rows_of(j), cols_of(c)], b_sem.at[j, c]
        )

    def a_copy(j):
        return pltpu.make_async_copy(band.at[j], a32.at[j], a_sem.at[j])

    for j in edge:
        m_copy(j).start()
    for c in range(chunks):
        for j in edge:
            b_copy(j, c).start()
    for j in inner_flat:
        m_copy(j).start()
    for c in range(chunks):
        for j in inner_flat:
            b_copy(j, c).start()
    for j in (*edge, *inner_flat):
        a_copy(j).start()

    barrier = pltpu.get_barrier_semaphore()
    for k in range(1, LINE):
        pl.semaphore_signal(
            barrier, inc=1, device_id={"rows": line * LINE + (spot + k) % LINE}, device_id_type=MESH
        )
    for k in range(1, lines):
        pl.semaphore_signal(
            barrier, inc=1, device_id={"rows": (line + k) % lines * LINE + spot}, device_id_type=MESH
        )
    for k in range(1, rhs_n):
        pl.semaphore_signal(barrier, inc=1, device_id={"rhs": (z + k) % rhs_n}, device_id_type=MESH)
    for side in range(2):

        @pl.when(far[side])
        def _():
            pl.semaphore_signal(barrier, inc=1, device_id={"rows": beside[side]}, device_id_type=MESH)

    peers = LINE - 1 + lines - 1 + rhs_n - 1

    part[...] = jnp.zeros_like(part)
    for side in range(2):

        @pl.when(jnp.logical_not(has[side]))
        def _():
            halo[:, :, side] = jnp.zeros_like(halo[:, :, side])

    def body(*accs):
        acc = (accs[:2], accs[2:])
        turn = [0]

        def products(jobs):
            pick = turn[0] % 2
            turn[0] += 1
            for step in range(max(len(job) for job in jobs)):
                for unit in range(2):
                    if step < len(jobs[unit]):
                        pltpu.matmul_push_rhs(
                            jobs[unit][step][0][...], staging_register=step % 2, mxu_index=unit
                        )
                for unit in range(2):
                    if step < len(jobs[unit]):
                        staged = step % 2
                        for left in jobs[unit][step][1]:
                            pltpu.matmul_acc_lhs(acc[unit][pick], left[...], load_staged_rhs=staged)
                            staged = None
            return [pltpu.matmul_pop(acc[unit][pick]) for unit in range(2)]

        def terms(left_high, left_low, right_high, right_low):
            return [(right_high, (left_high, left_low)), (right_low, (left_high,))]

        def band_terms(i, k, right_high, right_low):
            cut = (i, slice(None), slice(k * T, (k + 1) * T))
            return terms(ahi.at[cut], alo.at[cut], right_high, right_low)

        def precondition(pairs, c, first):
            for pair in pairs:
                values = products(
                    [terms(mhi.at[j], mlo.at[j], rhi.at[c, j], rlo.at[c, j]) for j in pair]
                )
                for j, value in zip(pair, values):
                    where = (rows_of(j), cols_of(c))
                    if first:
                        x[where] = value
                    else:
                        x[where] = x[where] + value
                    dhi[c, j], dlo[c, j] = split(value)
                    if j < 2:
                        dsend[c, 0, j] = value
                    elif j >= blocks - 2:
                        dsend[c, 1, j - (blocks - 2)] = value

        def settle(s, c, j, value, keep):
            where = (rows_of(j), cols_of(c))
            value = r[where] - value
            r[where] = value
            if keep:
                rhi[c, j], rlo[c, j] = split(value)
            return value

        def squares(s, c, values):
            total = part[s, c]
            for value in values:
                total = total + jnp.sum((value * value).reshape(T // 8, 8, T), axis=0)
            part[s, c] = total

        def local(s, c):
            for pair in zip(*((0, 1, *inner[0]), (blocks - 1, blocks - 2, *inner[1]))):
                jobs = []
                for i in pair:
                    job = []
                    for k in range(5):
                        j = i + k - 2
                        if 0 <= j < blocks:
                            job += band_terms(i, k, dhi.at[c, j], dlo.at[c, j])
                    jobs.append(job)
                values = products(jobs)
                for i, value in zip(pair, values):
                    if i in edge:
                        where = (rows_of(i), cols_of(c))
                        r[where] = r[where] - value
                    else:
                        squares(s, c, [settle(s, c, i, value, True)])

        def halo_copy(s, c, side):
            return pltpu.make_async_remote_copy(
                src_ref=dsend.at[c, side],
                dst_ref=halo.at[s, c, 1 - side],
                send_sem=send_sem.at[s, c, side],
                recv_sem=recv_sem.at[s, c, 1 - side],
                device_id={"rows": beside[side]},
                device_id_type=MESH,
            )

        def send(s, c):
            for side in range(2):

                @pl.when(has[side])
                def _():
                    halo_copy(s, c, side).start()

        def sent(s, c):
            for side in range(2):

                @pl.when(has[side])
                def _():
                    halo_copy(s, c, side).wait_send()

        def remote(s, c, keep):
            for side in range(2):

                @pl.when(has[side])
                def _():
                    pltpu.make_async_remote_copy(
                        src_ref=dsend.at[c, side],
                        dst_ref=halo.at[s, c, side],
                        send_sem=send_sem.at[s, c, side],
                        recv_sem=recv_sem.at[s, c, side],
                        device_id={"rows": beside[side]},
                        device_id_type=MESH,
                    ).wait_recv()

            for side in range(2):
                for q in range(2):
                    hhi[side, q], hlo[side, q] = split(halo[s, c, side, q])
            low = lambda q: (hhi.at[0, q], hlo.at[0, q])
            high = lambda q: (hhi.at[1, q], hlo.at[1, q])
            for pair, jobs in (
                (
                    (0, blocks - 1),
                    (
                        band_terms(0, 0, *low(0)) + band_terms(0, 1, *low(1)),
                        band_terms(blocks - 1, 3, *high(0)) + band_terms(blocks - 1, 4, *high(1)),
                    ),
                ),
                (
                    (1, blocks - 2),
                    (band_terms(1, 0, *low(1)), band_terms(blocks - 2, 4, *high(0))),
                ),
            ):
                values = products(jobs)
                squares(s, c, [settle(s, c, i, value, keep) for i, value in zip(pair, values)])

        def p1_copy(s, c, k):
            return pltpu.make_async_remote_copy(
                src_ref=msg.at[s, c],
                dst_ref=p1.at[s, c, k],
                send_sem=p1_send.at[s, c, k],
                recv_sem=p1_recv.at[s, c, k],
                device_id={"rows": line * LINE + (spot + k) % LINE},
                device_id_type=MESH,
            )

        def p2_copy(s, c, k):
            return pltpu.make_async_remote_copy(
                src_ref=mid.at[s, c],
                dst_ref=p2.at[s, c, k],
                send_sem=p2_send.at[s, c, k],
                recv_sem=p2_recv.at[s, c, k],
                device_id={"rows": (line + k) % lines * LINE + spot},
                device_id_type=MESH,
            )

        def sum_line(s, c):
            msg[s, c] = jnp.sum(part[s, c], axis=0, keepdims=True)
            for k in range(1, LINE):
                p1_copy(s, c, k).start()

        def sum_lines(s, c):
            total = msg[s, c]
            for k in range(1, LINE):
                p1_copy(s, c, k).wait()
                total = total + p1[s, c, k]
            mid[s, c] = total
            for k in range(1, lines):
                p2_copy(s, c, k).start()

        def summed(s, c):
            total = mid[s, c]
            for k in range(1, lines):
                p2_copy(s, c, k).wait()
                total = total + p2[s, c, k]
            return total

        def ready_rhs(js, c):
            for j in js:
                b_copy(j, c).wait()
                rhi[c, j], rlo[c, j] = split(r[rows_of(j), cols_of(c)])

        def ready_precond(js):
            for j in js:
                m_copy(j).wait()
                mhi[j], mlo[j] = split(m32[j])

        edge_pairs = ((0, blocks - 1), (1, blocks - 2))
        inner_pairs = tuple(zip(*inner))

        ready_precond(edge)
        for c in range(chunks):
            ready_rhs(edge, c)
            precondition(edge_pairs, c, True)
            if c == 0:
                pl.semaphore_wait(
                    barrier, peers + far[0].astype(jnp.int32) + far[1].astype(jnp.int32)
                )
            send(0, c)
        ready_precond(inner_flat)
        for c in range(chunks):
            ready_rhs(inner_flat, c)
            precondition(inner_pairs, c, True)
        for j in (*edge, *inner_flat):
            a_copy(j).wait()
            ahi[j], alo[j] = split(a32[j])

        def first_local(c, carry):
            local(0, c)
            return carry

        lax.fori_loop(0, chunks, first_local, 0)

        def unit(u, carry):
            s, c = u // chunks, u % chunks
            remote(s, c, True)
            sent(s, c)
            precondition(edge_pairs, c, False)
            send(s + 1, c)
            sum_line(s, c)
            precondition(inner_pairs, c, False)
            local(s + 1, c)
            sum_lines(s, c)
            return carry

        lax.fori_loop(0, (SWEEPS - 1) * chunks, unit, 0)

        last = SWEEPS - 1
        for c in range(chunks):
            remote(last, c, False)
            sum_line(last, c)
            sent(last, c)
            if c > 0:
                sum_lines(last, c - 1)
        sum_lines(last, chunks - 1)
        for s in range(SWEEPS - 1):
            for c in range(chunks):
                history[s : s + 1, cols_of(c)] = jnp.sqrt(
                    summed(s, c) / (rows_n * blocks * T) + 1e-06
                )
        grand = jnp.zeros((1, 1), F32)
        roots = []
        for c in range(chunks):
            total = summed(last, c)
            grand = grand + jnp.sum(total, axis=1, keepdims=True)
            root = jnp.sqrt(total / (rows_n * blocks * T) + 1e-06)
            history[last : last + 1, cols_of(c)] = root
            roots.append(root)
        zmsg[...] = jnp.broadcast_to(grand, zmsg.shape)

        def z_copy(k):
            return pltpu.make_async_remote_copy(
                src_ref=zmsg,
                dst_ref=zbuf.at[k],
                send_sem=z_send.at[k],
                recv_sem=z_recv.at[k],
                device_id={"rhs": (z + k) % rhs_n},
                device_id_type=MESH,
            )

        for k in range(1, rhs_n):
            z_copy(k).start()
        for c in range(chunks):
            inverse = 1.0 / roots[c]
            for j in range(blocks):
                where = (rows_of(j), cols_of(c))
                r[where] = r[where] * inverse
        grand = zmsg[...]
        for k in range(1, rhs_n):
            z_copy(k).wait()
            grand = grand + zbuf[k]
        overall[...] = jnp.sqrt(grand / (rows_n * blocks * T * rhs_n * rhs.shape[1]) + 1e-06)

    pl.run_scoped(body, *([pltpu.ACC(0)((T, T), F32)] * 2), *([pltpu.ACC(1)((T, T), F32)] * 2))


def shards(rows_n, rhs_n, band_blocks, precond_blocks, right_side):
    blocks = band_blocks.shape[0]
    n_rows, n_cols = right_side.shape
    chunks = n_cols // T
    band_blocks, precond_blocks, right_side = (
        pltpu.with_memory_space_constraint(v, pltpu.HBM) for v in (band_blocks, precond_blocks, right_side)
    )
    dma = pltpu.SemaphoreType.DMA
    vmem = pltpu.VMEM
    x, r, history, overall = pl.pallas_call(
        functools.partial(kernel, rows_n, rhs_n, blocks),
        out_shape=(
            vmem((n_rows, n_cols), F32),
            vmem((n_rows, n_cols), F32),
            jax.ShapeDtypeStruct((SWEEPS, n_cols), F32),
            jax.ShapeDtypeStruct((1, 128), F32),
        ),
        in_specs=[pl.BlockSpec(memory_space=pltpu.HBM)] * 3,
        out_specs=[pl.BlockSpec(memory_space=vmem)] * 4,
        scratch_shapes=[
            vmem((blocks, T, 5 * T), F32),
            vmem((blocks, T, T), F32),
            vmem((blocks, T, 5 * T), BF16),
            vmem((blocks, T, 5 * T), BF16),
            vmem((blocks, T, T), BF16),
            vmem((blocks, T, T), BF16),
            vmem((chunks, blocks, T, T), BF16),
            vmem((chunks, blocks, T, T), BF16),
            vmem((chunks, blocks, T, T), BF16),
            vmem((chunks, blocks, T, T), BF16),
            vmem((chunks, 2, 2, T, T), F32),
            vmem((SWEEPS, chunks, 2, 2, T, T), F32),
            vmem((2, 2, T, T), BF16),
            vmem((2, 2, T, T), BF16),
            vmem((SWEEPS, chunks, 8, T), F32),
            vmem((SWEEPS, chunks, 1, T), F32),
            vmem((SWEEPS, chunks, LINE, 1, T), F32),
            vmem((SWEEPS, chunks, 1, T), F32),
            vmem((SWEEPS, chunks, rows_n // LINE, 1, T), F32),
            vmem((1, 128), F32),
            vmem((rhs_n, 1, 128), F32),
            dma((blocks,)),
            dma((blocks,)),
            dma((blocks, chunks)),
            dma((SWEEPS, chunks, 2)),
            dma((SWEEPS, chunks, 2)),
            dma((SWEEPS, chunks, LINE)),
            dma((SWEEPS, chunks, LINE)),
            dma((SWEEPS, chunks, rows_n // LINE)),
            dma((SWEEPS, chunks, rows_n // LINE)),
            dma((rhs_n,)),
            dma((rhs_n,)),
        ],
        compiler_params=pltpu.CompilerParams(
            collective_id=0, has_side_effects=True, vmem_limit_bytes=50 * 1024 * 1024
        ),
        name="refine",
    )(band_blocks, precond_blocks, right_side)
    return x, r, history, overall[0, 0]


def solution(mesh):
    rows_n, rhs_n = mesh.shape["rows"], mesh.shape["rhs"]
    in_specs = (P("rows", None, None), P("rows", None, None), P("rows", "rhs"))
    out_specs = (P("rows", "rhs"), P("rows", "rhs"), P(None, "rhs"), P())
    return jax.shard_map(
        functools.partial(shards, rows_n, rhs_n),
        mesh=mesh,
        in_specs=in_specs,
        out_specs=out_specs,
        check_vma=False,
    )
```

```python
import functools

import jax
import jax.numpy as jnp
from jax import lax
from jax.experimental import pallas as pl
from jax.experimental.pallas import tpu as pltpu
from jax.sharding import PartitionSpec as P

MESH = pl.DeviceIdType.MESH
F32, BF16 = jnp.float32, jnp.bfloat16
SWEEPS = 3
T = 256
PIECES = 4
LINE = 8


def split(value):
    high = value.astype(BF16)
    return high, (value - high.astype(F32)).astype(BF16)


def kernel(
    rows_n, rhs_n, blocks,
    band, precond, rhs,
    x, r, history, overall,
    a32, m32, ahi, alo, mhi, mlo, rhi, rlo, dhi, dlo, dsend, halo, hhi, hlo, part, msg, p1, mid, p2, zmsg, zbuf,
    a_sem, m_sem, b_sem, send_sem, recv_sem, p1_send, p1_recv, p2_send, p2_recv, z_send, z_recv,
):
    me = lax.axis_index("rows")
    z = lax.axis_index("rhs")
    lines = rows_n // LINE
    line, spot = me // LINE, me % LINE
    has = (me > 0, me < rows_n - 1)
    beside = (me - 1, me + 1)
    far = ((spot == 0) & has[0], (spot == LINE - 1) & has[1])
    chunks = rhs.shape[1] // T
    edge = (0, 1, blocks - 1, blocks - 2)
    inner = tuple(range(2, blocks // 2)), tuple(range(blocks - 3, blocks // 2 - 1, -1))
    inner_flat = tuple(j for pair in zip(*inner) for j in pair)

    def rows_of(j):
        return slice(j * T, (j + 1) * T)

    def cols_of(c):
        if isinstance(c, int):
            return slice(c * T, (c + 1) * T)
        return pl.ds(pl.multiple_of(c * T, T), T)

    def m_copy(j):
        return pltpu.make_async_copy(precond.at[j], m32.at[j], m_sem.at[j])

    def b_copy(j, c):
        return pltpu.make_async_copy(
            rhs.at[rows_of(j), cols_of(c)], r.at[rows_of(j), cols_of(c)], b_sem.at[j, c]
        )

    def a_copy(j):
        return pltpu.make_async_copy(band.at[j], a32.at[j], a_sem.at[j])

    for j in edge:
        m_copy(j).start()
    for c in range(chunks):
        for j in edge:
            b_copy(j, c).start()
    for j in inner_flat:
        m_copy(j).start()
    for c in range(chunks):
        for j in inner_flat:
            b_copy(j, c).start()
    band_pairs = tuple(zip((0, 1, *inner[0]), (blocks - 1, blocks - 2, *inner[1])))
    for pair in band_pairs:
        for j in pair:
            a_copy(j).start()

    barrier = pltpu.get_barrier_semaphore()
    for k in range(1, LINE):
        pl.semaphore_signal(
            barrier, inc=1, device_id={"rows": line * LINE + (spot + k) % LINE}, device_id_type=MESH
        )
    for k in range(1, lines):
        pl.semaphore_signal(
            barrier, inc=1, device_id={"rows": (line + k) % lines * LINE + spot}, device_id_type=MESH
        )
    for k in range(1, rhs_n):
        pl.semaphore_signal(barrier, inc=1, device_id={"rhs": (z + k) % rhs_n}, device_id_type=MESH)
    for side in range(2):

        @pl.when(far[side])
        def _():
            pl.semaphore_signal(barrier, inc=1, device_id={"rows": beside[side]}, device_id_type=MESH)

    peers = LINE - 1 + lines - 1 + rhs_n - 1

    def body(*accs):
        acc = (accs[:2], accs[2:])
        turn = [0]

        def products(jobs):
            pick = turn[0] % 2
            turn[0] += 1
            for step in range(max(len(job) for job in jobs)):
                for unit in range(2):
                    if step < len(jobs[unit]):
                        pltpu.matmul_push_rhs(
                            jobs[unit][step][0][...], staging_register=step % 2, mxu_index=unit
                        )
                for unit in range(2):
                    if step < len(jobs[unit]):
                        staged = step % 2
                        for left in jobs[unit][step][1]:
                            pltpu.matmul_acc_lhs(acc[unit][pick], left[...], load_staged_rhs=staged)
                            staged = None
            return [pltpu.matmul_pop(acc[unit][pick]) for unit in range(2)]

        def terms(left_high, left_low, right_high, right_low):
            return [(right_high, (left_high, left_low)), (right_low, (left_high,))]

        def band_terms(i, k, right_high, right_low):
            cut = (i, slice(None), slice(k * T, (k + 1) * T))
            return terms(ahi.at[cut], alo.at[cut], right_high, right_low)

        def precondition(pairs, s, c, first):
            for pair in pairs:
                values = products(
                    [terms(mhi.at[j], mlo.at[j], rhi.at[c, j], rlo.at[c, j]) for j in pair]
                )
                for j, value in zip(pair, values):
                    where = (rows_of(j), cols_of(c))
                    if first:
                        x[where] = value
                    else:
                        x[where] = x[where] + value
                    dhi[c, j], dlo[c, j] = split(value)
                    if j < 2:
                        dsend[s, c, 0, j] = value
                    elif j >= blocks - 2:
                        dsend[s, c, 1, j - (blocks - 2)] = value

        def settle(s, c, j, value, keep):
            where = (rows_of(j), cols_of(c))
            value = r[where] - value
            r[where] = value
            if keep:
                rhi[c, j], rlo[c, j] = split(value)
            return value

        def squares(s, c, values):
            total = part[s, c]
            for value in values:
                total = total + jnp.sum((value * value).reshape(T // 8, 8, T), axis=0)
            part[s, c] = total

        def local(s, c, pairs):
            for pair in pairs:
                jobs = []
                for i in pair:
                    job = []
                    for k in range(5):
                        j = i + k - 2
                        if 0 <= j < blocks:
                            job += band_terms(i, k, dhi.at[c, j], dlo.at[c, j])
                    jobs.append(job)
                values = products(jobs)
                for i, value in zip(pair, values):
                    if i in edge:
                        where = (rows_of(i), cols_of(c))
                        r[where] = r[where] - value
                    else:
                        squares(s, c, [settle(s, c, i, value, True)])

        def halo_copy(s, c, side):
            return pltpu.make_async_remote_copy(
                src_ref=dsend.at[s, c, side],
                dst_ref=halo.at[s, c, 1 - side],
                send_sem=send_sem.at[s, c, side],
                recv_sem=recv_sem.at[s, c, 1 - side],
                device_id={"rows": beside[side]},
                device_id_type=MESH,
            )

        def send(s, c):
            for side in range(2):

                @pl.when(has[side])
                def _():
                    halo_copy(s, c, side).start()

        def sent(s, c):
            for side in range(2):

                @pl.when(has[side])
                def _():
                    halo_copy(s, c, side).wait_send()

        def arrive(s, c):
            for side in range(2):

                @pl.when(has[side])
                def _():
                    pltpu.make_async_remote_copy(
                        src_ref=dsend.at[s, c, side],
                        dst_ref=halo.at[s, c, side],
                        send_sem=send_sem.at[s, c, side],
                        recv_sem=recv_sem.at[s, c, side],
                        device_id={"rows": beside[side]},
                        device_id_type=MESH,
                    ).wait_recv()

        def remote(s, c, keep):
            for side in range(2):
                for q in range(2):
                    hhi[side, q], hlo[side, q] = split(halo[s, c, side, q])
            low = lambda q: (hhi.at[0, q], hlo.at[0, q])
            high = lambda q: (hhi.at[1, q], hlo.at[1, q])
            for pair, jobs in (
                (
                    (0, blocks - 1),
                    (
                        band_terms(0, 0, *low(0)) + band_terms(0, 1, *low(1)),
                        band_terms(blocks - 1, 3, *high(0)) + band_terms(blocks - 1, 4, *high(1)),
                    ),
                ),
                (
                    (1, blocks - 2),
                    (band_terms(1, 0, *low(1)), band_terms(blocks - 2, 4, *high(0))),
                ),
            ):
                values = products(jobs)
                squares(s, c, [settle(s, c, i, value, keep) for i, value in zip(pair, values)])

        def p1_copy(s, c, k):
            return pltpu.make_async_remote_copy(
                src_ref=msg.at[s, c],
                dst_ref=p1.at[s, c, k],
                send_sem=p1_send.at[s, c, k],
                recv_sem=p1_recv.at[s, c, k],
                device_id={"rows": line * LINE + (spot + k) % LINE},
                device_id_type=MESH,
            )

        def p2_copy(s, c, k):
            return pltpu.make_async_remote_copy(
                src_ref=mid.at[s, c],
                dst_ref=p2.at[s, c, k],
                send_sem=p2_send.at[s, c, k],
                recv_sem=p2_recv.at[s, c, k],
                device_id={"rows": (line + k) % lines * LINE + spot},
                device_id_type=MESH,
            )

        def sum_line(s, c):
            msg[s, c] = jnp.sum(part[s, c], axis=0, keepdims=True)
            for k in range(1, LINE):
                p1_copy(s, c, k).start()

        def sum_lines(s, c):
            total = msg[s, c]
            for k in range(1, LINE):
                p1_copy(s, c, k).wait()
                total = total + p1[s, c, k]
            mid[s, c] = total
            for k in range(1, lines):
                p2_copy(s, c, k).start()

        def summed(s, c):
            total = mid[s, c]
            for k in range(1, lines):
                p2_copy(s, c, k).wait()
                total = total + p2[s, c, k]
            return total

        def ready_rhs(js, c):
            for j in js:
                b_copy(j, c).wait()
                rhi[c, j], rlo[c, j] = split(r[rows_of(j), cols_of(c)])

        def ready_precond(js):
            for j in js:
                m_copy(j).wait()
                mhi[j], mlo[j] = split(m32[j])

        edge_pairs = ((0, blocks - 1), (1, blocks - 2))
        inner_pairs = tuple(zip(*inner))

        def ready_band(js):
            for j in js:
                a_copy(j).wait()
            for j in js:
                ahi[j], alo[j] = split(a32[j])

        ready_precond(edge)
        for c in range(chunks):
            ready_rhs(edge, c)
            precondition(edge_pairs, 0, c, True)
            if c == 0:
                pl.semaphore_wait(
                    barrier, peers + far[0].astype(jnp.int32) + far[1].astype(jnp.int32)
                )
            send(0, c)
        part[...] = jnp.zeros_like(part)
        for side in range(2):

            @pl.when(jnp.logical_not(has[side]))
            def _():
                halo[:, :, side] = jnp.zeros_like(halo[:, :, side])

        for j in inner_flat:
            m_copy(j).wait()
            for c in range(chunks):
                b_copy(j, c).wait()
        for j in inner_flat:
            mhi[j], mlo[j] = split(m32[j])
        for c in range(chunks):
            for j in inner_flat:
                rhi[c, j], rlo[c, j] = split(r[rows_of(j), cols_of(c)])
            precondition(inner_pairs, 0, c, True)
        ready_band(band_pairs[0])
        for n, pair in enumerate(band_pairs):
            if n + 1 < len(band_pairs):
                ready_band(band_pairs[n + 1])
            for c in range(chunks):
                local(0, c, (pair,))

        def unit(u, carry):
            s, c = u // chunks, u % chunks
            precondition(inner_pairs[:1], s + 1, c, False)
            arrive(s, c)
            remote(s, c, True)
            precondition(inner_pairs[1:], s + 1, c, False)
            precondition(edge_pairs, s + 1, c, False)
            sum_line(s, c)
            send(s + 1, c)
            local(s + 1, c, band_pairs[::-1])
            return carry

        lax.fori_loop(0, (SWEEPS - 1) * chunks, unit, 0)

        last = SWEEPS - 1
        earlier = [(s, c) for s in range(last) for c in range(chunks)]
        for c in range(chunks):
            arrive(last, c)
            remote(last, c, False)
            sum_line(last, c)
            if c == 0:
                for s, other in earlier:
                    sum_lines(s, other)
        for c in range(chunks):
            sum_lines(last, c)
        for s in range(SWEEPS):
            for c in range(chunks):
                sent(s, c)
        for s, c in earlier:
            history[s : s + 1, cols_of(c)] = jnp.sqrt(summed(s, c) / (rows_n * blocks * T) + 1e-06)
        grand = jnp.zeros((1, 1), F32)
        roots = []
        for c in range(chunks):
            total = summed(last, c)
            grand = grand + jnp.sum(total, axis=1, keepdims=True)
            root = jnp.sqrt(total / (rows_n * blocks * T) + 1e-06)
            history[last : last + 1, cols_of(c)] = root
            roots.append(root)
        zmsg[...] = jnp.broadcast_to(grand, zmsg.shape)

        def z_copy(k):
            return pltpu.make_async_remote_copy(
                src_ref=zmsg,
                dst_ref=zbuf.at[k],
                send_sem=z_send.at[k],
                recv_sem=z_recv.at[k],
                device_id={"rhs": (z + k) % rhs_n},
                device_id_type=MESH,
            )

        for k in range(1, rhs_n):
            z_copy(k).start()
        for c in range(chunks):
            inverse = 1.0 / roots[c]
            for j in range(blocks):
                where = (rows_of(j), cols_of(c))
                r[where] = r[where] * inverse
        grand = zmsg[...]
        for k in range(1, rhs_n):
            z_copy(k).wait()
            grand = grand + zbuf[k]
        overall[...] = jnp.sqrt(grand / (rows_n * blocks * T * rhs_n * rhs.shape[1]) + 1e-06)

    pl.run_scoped(body, *([pltpu.ACC(0)((T, T), F32)] * 2), *([pltpu.ACC(1)((T, T), F32)] * 2))


def write_out(x, r, history, overall, x_out, r_out, history_out, overall_out, sem, small_sem):
    height = x.shape[0] // PIECES
    copies = [
        pltpu.make_async_copy(history, history_out, small_sem.at[0]),
        pltpu.make_async_copy(overall, overall_out, small_sem.at[1]),
    ]
    for n in range(PIECES):
        rows = slice(n * height, (n + 1) * height)
        copies.append(pltpu.make_async_copy(x.at[rows], x_out.at[rows], sem.at[0, n]))
        copies.append(pltpu.make_async_copy(r.at[rows], r_out.at[rows], sem.at[1, n]))
    for copy in copies:
        copy.start()
    for copy in copies:
        copy.wait()


def shards(rows_n, rhs_n, band_blocks, precond_blocks, right_side):
    blocks = band_blocks.shape[0]
    n_rows, n_cols = right_side.shape
    chunks = n_cols // T
    band_blocks, precond_blocks, right_side = (
        pltpu.with_memory_space_constraint(v, pltpu.HBM) for v in (band_blocks, precond_blocks, right_side)
    )
    dma = pltpu.SemaphoreType.DMA
    vmem = pltpu.VMEM
    x, r, history, overall = pl.pallas_call(
        functools.partial(kernel, rows_n, rhs_n, blocks),
        out_shape=(
            vmem((n_rows, n_cols), F32),
            vmem((n_rows, n_cols), F32),
            vmem((SWEEPS, n_cols), F32),
            vmem((1, 128), F32),
        ),
        in_specs=[pl.BlockSpec(memory_space=pltpu.HBM)] * 3,
        out_specs=[pl.BlockSpec(memory_space=vmem)] * 4,
        scratch_shapes=[
            vmem((blocks, T, 5 * T), F32),
            vmem((blocks, T, T), F32),
            vmem((blocks, T, 5 * T), BF16),
            vmem((blocks, T, 5 * T), BF16),
            vmem((blocks, T, T), BF16),
            vmem((blocks, T, T), BF16),
            vmem((chunks, blocks, T, T), BF16),
            vmem((chunks, blocks, T, T), BF16),
            vmem((chunks, blocks, T, T), BF16),
            vmem((chunks, blocks, T, T), BF16),
            vmem((SWEEPS, chunks, 2, 2, T, T), F32),
            vmem((SWEEPS, chunks, 2, 2, T, T), F32),
            vmem((2, 2, T, T), BF16),
            vmem((2, 2, T, T), BF16),
            vmem((SWEEPS, chunks, 8, T), F32),
            vmem((SWEEPS, chunks, 1, T), F32),
            vmem((SWEEPS, chunks, LINE, 1, T), F32),
            vmem((SWEEPS, chunks, 1, T), F32),
            vmem((SWEEPS, chunks, rows_n // LINE, 1, T), F32),
            vmem((1, 128), F32),
            vmem((rhs_n, 1, 128), F32),
            dma((blocks,)),
            dma((blocks,)),
            dma((blocks, chunks)),
            dma((SWEEPS, chunks, 2)),
            dma((SWEEPS, chunks, 2)),
            dma((SWEEPS, chunks, LINE)),
            dma((SWEEPS, chunks, LINE)),
            dma((SWEEPS, chunks, rows_n // LINE)),
            dma((SWEEPS, chunks, rows_n // LINE)),
            dma((rhs_n,)),
            dma((rhs_n,)),
        ],
        compiler_params=pltpu.CompilerParams(
            collective_id=0, has_side_effects=True, vmem_limit_bytes=54 * 1024 * 1024
        ),
        name="refine",
    )(band_blocks, precond_blocks, right_side)
    x, r, history, overall = pl.pallas_call(
        write_out,
        out_shape=(
            jax.ShapeDtypeStruct((n_rows, n_cols), F32),
            jax.ShapeDtypeStruct((n_rows, n_cols), F32),
            jax.ShapeDtypeStruct((SWEEPS, n_cols), F32),
            jax.ShapeDtypeStruct((1, 128), F32),
        ),
        in_specs=[pl.BlockSpec(memory_space=vmem)] * 4,
        out_specs=[pl.BlockSpec(memory_space=pltpu.HBM)] * 4,
        scratch_shapes=[dma((2, PIECES)), dma((2,))],
        compiler_params=pltpu.CompilerParams(vmem_limit_bytes=1024 * 1024),
        name="write_out",
    )(x, r, history, overall)
    return x, r, history, overall[0, 0]


def solution(mesh):
    rows_n, rhs_n = mesh.shape["rows"], mesh.shape["rhs"]
    in_specs = (P("rows", None, None), P("rows", None, None), P("rows", "rhs"))
    out_specs = (P("rows", "rhs"), P("rows", "rhs"), P(None, "rhs"), P())
    return jax.shard_map(
        functools.partial(shards, rows_n, rhs_n),
        mesh=mesh,
        in_specs=in_specs,
        out_specs=out_specs,
        check_vma=False,
    )
```

```python
import functools

import jax
import jax.numpy as jnp
from jax import lax
from jax.experimental import pallas as pl
from jax.experimental.pallas import tpu as pltpu
from jax.sharding import PartitionSpec as P

MESH = pl.DeviceIdType.MESH
F32, BF16 = jnp.float32, jnp.bfloat16
SWEEPS = 3
T = 256
PIECES = 4
LINE = 8


def split(value):
    high = value.astype(BF16)
    return high, (value - high.astype(F32)).astype(BF16)


def kernel(
    rows_n, rhs_n, blocks,
    band, precond, rhs,
    x, r, history, overall,
    a32, m32, ahi, alo, mhi, mlo, rhi, rlo, dhi, dlo, dsend, halo, hhi, hlo, part, msg, p1, mid, p2, zmsg, zbuf,
    ready, last_msg, last_all, last_send, last_recv,
    a_sem, m_sem, b_sem, send_sem, recv_sem, p1_send, p1_recv, p2_send, p2_recv, z_send, z_recv,
):
    me = lax.axis_index("rows")
    z = lax.axis_index("rhs")
    lines = rows_n // LINE
    line, spot = me // LINE, me % LINE
    has = (me > 0, me < rows_n - 1)
    beside = (me - 1, me + 1)
    far = ((spot == 0) & has[0], (spot == LINE - 1) & has[1])
    chunks = rhs.shape[1] // T
    assert chunks == 2
    edge = (0, 1, blocks - 1, blocks - 2)
    inner = tuple(range(2, blocks // 2)), tuple(range(blocks - 3, blocks // 2 - 1, -1))
    inner_flat = tuple(j for pair in zip(*inner) for j in pair)

    def rows_of(j):
        return slice(j * T, (j + 1) * T)

    def cols_of(c):
        if isinstance(c, int):
            return slice(c * T, (c + 1) * T)
        return pl.ds(pl.multiple_of(c * T, T), T)

    def m_copy(j):
        return pltpu.make_async_copy(precond.at[j], m32.at[j], m_sem.at[j])

    def b_copy(j, c):
        return pltpu.make_async_copy(
            rhs.at[rows_of(j), cols_of(c)], r.at[rows_of(j), cols_of(c)], b_sem.at[j, c]
        )

    def a_copy(j):
        return pltpu.make_async_copy(band.at[j], a32.at[j], a_sem.at[j])

    for j in edge:
        m_copy(j).start()
    for c in range(chunks):
        for j in edge:
            b_copy(j, c).start(priority=min(c, 1))
    for j in inner_flat:
        m_copy(j).start(priority=1)
    for c in range(chunks):
        for j in inner_flat:
            b_copy(j, c).start(priority=1)
    band_pairs = tuple(zip((0, 1, *inner[0]), (blocks - 1, blocks - 2, *inner[1])))
    for pair in band_pairs:
        for j in pair:
            a_copy(j).start(priority=1)

    barrier = pltpu.get_barrier_semaphore()
    for k in range(1, LINE):
        pl.semaphore_signal(
            barrier, inc=1, device_id={"rows": line * LINE + (spot + k) % LINE}, device_id_type=MESH
        )
    for k in range(1, lines):
        pl.semaphore_signal(
            barrier, inc=1, device_id={"rows": (line + k) % lines * LINE + spot}, device_id_type=MESH
        )
    for k in range(1, rhs_n):
        pl.semaphore_signal(barrier, inc=1, device_id={"rhs": (z + k) % rhs_n}, device_id_type=MESH)
    for side in range(2):

        @pl.when(far[side])
        def _():
            pl.semaphore_signal(barrier, inc=1, device_id={"rows": beside[side]}, device_id_type=MESH)

    peers = LINE - 1 + lines - 1 + rhs_n - 1

    def body(*accs):
        acc = (accs[:2], accs[2:])
        turn = [0]

        def products(jobs):
            pick = turn[0] % 2
            turn[0] += 1
            for step in range(max(len(job) for job in jobs)):
                for unit in range(2):
                    if step < len(jobs[unit]):
                        pltpu.matmul_push_rhs(
                            jobs[unit][step][0][...], staging_register=step % 2, mxu_index=unit
                        )
                for unit in range(2):
                    if step < len(jobs[unit]):
                        staged = step % 2
                        for left in jobs[unit][step][1]:
                            pltpu.matmul_acc_lhs(acc[unit][pick], left[...], load_staged_rhs=staged)
                            staged = None
            return [pltpu.matmul_pop(acc[unit][pick]) for unit in range(2)]

        def terms(left_high, left_low, right_high, right_low):
            return [(right_high, (left_high, left_low)), (right_low, (left_high,))]

        def band_terms(i, k, right_high, right_low):
            cut = (i, slice(None), slice(k * T, (k + 1) * T))
            return terms(ahi.at[cut], alo.at[cut], right_high, right_low)

        def precondition(pairs, s, c, first):
            for pair in pairs:
                values = products(
                    [terms(mhi.at[j], mlo.at[j], rhi.at[c, j], rlo.at[c, j]) for j in pair]
                )
                for j, value in zip(pair, values):
                    where = (rows_of(j), cols_of(c))
                    if first:
                        x[where] = value
                    else:
                        x[where] = x[where] + value
                    dhi[c, j], dlo[c, j] = split(value)
                    if j < 2:
                        dsend[s, c, 0, j] = value
                    elif j >= blocks - 2:
                        dsend[s, c, 1, j - (blocks - 2)] = value

        def settle(s, c, j, value, keep):
            where = (rows_of(j), cols_of(c))
            value = r[where] - value
            r[where] = value
            if keep:
                rhi[c, j], rlo[c, j] = split(value)
            return value

        def squares(s, c, values):
            total = part[s, c]
            for value in values:
                total = total + jnp.sum((value * value).reshape(T // 8, 8, T), axis=0)
            part[s, c] = total

        def local(s, c, pairs):
            for pair in pairs:
                jobs = []
                for i in pair:
                    job = []
                    for k in range(5):
                        j = i + k - 2
                        if 0 <= j < blocks:
                            job += band_terms(i, k, dhi.at[c, j], dlo.at[c, j])
                    jobs.append(job)
                values = products(jobs)
                for i, value in zip(pair, values):
                    if i in edge:
                        where = (rows_of(i), cols_of(c))
                        r[where] = r[where] - value
                    else:
                        squares(s, c, [settle(s, c, i, value, True)])

        def halo_copy(s, c, side):
            return pltpu.make_async_remote_copy(
                src_ref=dsend.at[s, c, side],
                dst_ref=halo.at[s, c, 1 - side],
                send_sem=send_sem.at[s, c, side],
                recv_sem=recv_sem.at[s, c, 1 - side],
                device_id={"rows": beside[side]},
                device_id_type=MESH,
            )

        def send(s, c):
            for side in range(2):

                @pl.when(has[side])
                def _():
                    halo_copy(s, c, side).start()

        def sent(s, c):
            for side in range(2):

                @pl.when(has[side])
                def _():
                    halo_copy(s, c, side).wait_send()

        def arrive(s, c):
            for side in range(2):

                @pl.when(has[side])
                def _():
                    pltpu.make_async_remote_copy(
                        src_ref=dsend.at[s, c, side],
                        dst_ref=halo.at[s, c, side],
                        send_sem=send_sem.at[s, c, side],
                        recv_sem=recv_sem.at[s, c, side],
                        device_id={"rows": beside[side]},
                        device_id_type=MESH,
                    ).wait_recv()

        def remote(s, c, keep):
            for side in range(2):
                for q in range(2):
                    hhi[side, q], hlo[side, q] = split(halo[s, c, side, q])
            low = lambda q: (hhi.at[0, q], hlo.at[0, q])
            high = lambda q: (hhi.at[1, q], hlo.at[1, q])
            for pair, jobs in (
                (
                    (0, blocks - 1),
                    (
                        band_terms(0, 0, *low(0)) + band_terms(0, 1, *low(1)),
                        band_terms(blocks - 1, 3, *high(0)) + band_terms(blocks - 1, 4, *high(1)),
                    ),
                ),
                (
                    (1, blocks - 2),
                    (band_terms(1, 0, *low(1)), band_terms(blocks - 2, 4, *high(0))),
                ),
            ):
                values = products(jobs)
                squares(s, c, [settle(s, c, i, value, keep) for i, value in zip(pair, values)])

        def p1_copy(s, c, k):
            return pltpu.make_async_remote_copy(
                src_ref=msg.at[s, c],
                dst_ref=p1.at[s, c, k],
                send_sem=p1_send.at[s, c, k],
                recv_sem=p1_recv.at[s, c, k],
                device_id={"rows": line * LINE + (spot + k) % LINE},
                device_id_type=MESH,
            )

        def p2_copy(s, c, k):
            return pltpu.make_async_remote_copy(
                src_ref=mid.at[s, c],
                dst_ref=p2.at[s, c, k],
                send_sem=p2_send.at[s, c, k],
                recv_sem=p2_recv.at[s, c, k],
                device_id={"rows": (line + k) % lines * LINE + spot},
                device_id_type=MESH,
            )

        def sum_line(s, c):
            msg[s, c] = jnp.sum(part[s, c], axis=0, keepdims=True)
            for k in range(1, LINE):
                p1_copy(s, c, k).start()

        def sum_lines(s, c):
            total = msg[s, c]
            for k in range(1, LINE):
                p1_copy(s, c, k).wait()
                total = total + p1[s, c, k]
            mid[s, c] = total
            for k in range(1, lines):
                p2_copy(s, c, k).start()

        def summed(s, c):
            total = mid[s, c]
            for k in range(1, lines):
                p2_copy(s, c, k).wait()
                total = total + p2[s, c, k]
            return total

        def ready_rhs(js, c):
            for j in js:
                b_copy(j, c).wait()
                rhi[c, j], rlo[c, j] = split(r[rows_of(j), cols_of(c)])

        def ready_precond(js):
            for j in js:
                m_copy(j).wait()
                mhi[j], mlo[j] = split(m32[j])

        edge_pairs = ((0, blocks - 1), (1, blocks - 2))
        inner_pairs = tuple(zip(*inner))

        def ready_band(js):
            for j in js:
                a_copy(j).wait()
            for j in js:
                ahi[j], alo[j] = split(a32[j])

        ready_precond(edge)
        for c in range(chunks):
            ready_rhs(edge, c)
            precondition(edge_pairs, 0, c, True)
            if c == 0:
                pl.semaphore_wait(
                    barrier, peers + far[0].astype(jnp.int32) + far[1].astype(jnp.int32)
                )
            send(0, c)
        for k in range(1, LINE):
            pl.semaphore_signal(
                ready, inc=1, device_id={"rows": line * LINE + (spot + k) % LINE}, device_id_type=MESH
            )
        part[...] = jnp.zeros_like(part)
        for side in range(2):

            @pl.when(jnp.logical_not(has[side]))
            def _():
                halo[:, :, side] = jnp.zeros_like(halo[:, :, side])

        for j in inner_flat:
            m_copy(j).wait()
            for c in range(chunks):
                b_copy(j, c).wait()
        for j in inner_flat:
            mhi[j], mlo[j] = split(m32[j])
        for c in range(chunks):
            for j in inner_flat:
                rhi[c, j], rlo[c, j] = split(r[rows_of(j), cols_of(c)])
            precondition(inner_pairs, 0, c, True)
        ready_band(band_pairs[0])
        for n, pair in enumerate(band_pairs):
            if n + 1 < len(band_pairs):
                ready_band(band_pairs[n + 1])
            for c in range(chunks):
                if c == 0 or pair in edge_pairs:
                    local(0, c, (pair,))

        def unit(u, carry):
            s, c = u // chunks, u % chunks
            precondition(inner_pairs[:1], s + 1, c, False)
            arrive(s, c)
            remote(s, c, True)
            precondition(inner_pairs[1:], s + 1, c, False)
            precondition(edge_pairs, s + 1, c, False)
            sum_line(s, c)
            send(s + 1, c)
            local((u + 1) // chunks, 1 - c, inner_pairs[::-1])
            local(s + 1, c, edge_pairs[::-1])
            return carry

        lax.fori_loop(0, (SWEEPS - 1) * chunks, unit, 0)

        def last_copy(k):
            return pltpu.make_async_remote_copy(
                src_ref=last_msg,
                dst_ref=last_all.at[k],
                send_sem=last_send.at[k],
                recv_sem=last_recv.at[k],
                device_id={"rows": (me + k) % rows_n},
                device_id_type=MESH,
            )

        last = SWEEPS - 1
        earlier = [(s, c) for s in range(last) for c in range(chunks)]
        local(last, chunks - 1, inner_pairs)
        for c in range(chunks):
            arrive(last, c)
            remote(last, c, False)
            last_msg[:, cols_of(c)] = jnp.sum(part[last, c], axis=0, keepdims=True)
            if c == 0:
                pl.semaphore_wait(ready, LINE - 1)
                for s, other in earlier:
                    sum_lines(s, other)
        for k in range(1, rows_n):
            last_copy(k).start()
        for s in range(SWEEPS):
            for c in range(chunks):
                sent(s, c)
        for s, c in earlier:
            history[s : s + 1, cols_of(c)] = jnp.sqrt(summed(s, c) / (rows_n * blocks * T) + 1e-06)
        last_all[0] = last_msg[...]
        for k in range(1, rows_n):
            last_copy(k).wait()
        total = jnp.sum(last_all[...], axis=0)
        root = jnp.sqrt(total / (rows_n * blocks * T) + 1e-06)
        history[last : last + 1] = root
        grand = jnp.sum(total, axis=1, keepdims=True)
        zmsg[...] = jnp.broadcast_to(grand, zmsg.shape)

        def z_copy(k):
            return pltpu.make_async_remote_copy(
                src_ref=zmsg,
                dst_ref=zbuf.at[k],
                send_sem=z_send.at[k],
                recv_sem=z_recv.at[k],
                device_id={"rhs": (z + k) % rhs_n},
                device_id_type=MESH,
            )

        for k in range(1, rhs_n):
            z_copy(k).start()
        inverse = 1.0 / root
        for j in range(blocks):
            r[rows_of(j)] = r[rows_of(j)] * inverse
        grand = zmsg[...]
        for k in range(1, rhs_n):
            z_copy(k).wait()
            grand = grand + zbuf[k]
        overall[...] = jnp.sqrt(grand / (rows_n * blocks * T * rhs_n * rhs.shape[1]) + 1e-06)

    pl.run_scoped(body, *([pltpu.ACC(0)((T, T), F32)] * 2), *([pltpu.ACC(1)((T, T), F32)] * 2))


def write_out(x, r, history, overall, x_out, r_out, history_out, overall_out, sem, small_sem):
    height = x.shape[0] // PIECES
    copies = [
        pltpu.make_async_copy(history, history_out, small_sem.at[0]),
        pltpu.make_async_copy(overall, overall_out, small_sem.at[1]),
    ]
    for n in range(PIECES):
        rows = slice(n * height, (n + 1) * height)
        copies.append(pltpu.make_async_copy(x.at[rows], x_out.at[rows], sem.at[0, n]))
        copies.append(pltpu.make_async_copy(r.at[rows], r_out.at[rows], sem.at[1, n]))
    for copy in copies:
        copy.start()
    for copy in copies:
        copy.wait()


def shards(rows_n, rhs_n, band_blocks, precond_blocks, right_side):
    blocks = band_blocks.shape[0]
    n_rows, n_cols = right_side.shape
    chunks = n_cols // T
    band_blocks, precond_blocks, right_side = (
        pltpu.with_memory_space_constraint(v, pltpu.HBM) for v in (band_blocks, precond_blocks, right_side)
    )
    dma = pltpu.SemaphoreType.DMA
    vmem = pltpu.VMEM
    x, r, history, overall = pl.pallas_call(
        functools.partial(kernel, rows_n, rhs_n, blocks),
        out_shape=(
            vmem((n_rows, n_cols), F32),
            vmem((n_rows, n_cols), F32),
            vmem((SWEEPS, n_cols), F32),
            vmem((1, 128), F32),
        ),
        in_specs=[pl.BlockSpec(memory_space=pltpu.HBM)] * 3,
        out_specs=[pl.BlockSpec(memory_space=vmem)] * 4,
        scratch_shapes=[
            vmem((blocks, T, 5 * T), F32),
            vmem((blocks, T, T), F32),
            vmem((blocks, T, 5 * T), BF16),
            vmem((blocks, T, 5 * T), BF16),
            vmem((blocks, T, T), BF16),
            vmem((blocks, T, T), BF16),
            vmem((chunks, blocks, T, T), BF16),
            vmem((chunks, blocks, T, T), BF16),
            vmem((chunks, blocks, T, T), BF16),
            vmem((chunks, blocks, T, T), BF16),
            vmem((SWEEPS, chunks, 2, 2, T, T), F32),
            vmem((SWEEPS, chunks, 2, 2, T, T), F32),
            vmem((2, 2, T, T), BF16),
            vmem((2, 2, T, T), BF16),
            vmem((SWEEPS, chunks, 8, T), F32),
            vmem((SWEEPS, chunks, 1, T), F32),
            vmem((SWEEPS, chunks, LINE, 1, T), F32),
            vmem((SWEEPS, chunks, 1, T), F32),
            vmem((SWEEPS, chunks, rows_n // LINE, 1, T), F32),
            vmem((1, 128), F32),
            vmem((rhs_n, 1, 128), F32),
            pltpu.SemaphoreType.REGULAR,
            vmem((1, n_cols), F32),
            vmem((rows_n, 1, n_cols), F32),
            dma((rows_n,)),
            dma((rows_n,)),
            dma((blocks,)),
            dma((blocks,)),
            dma((blocks, chunks)),
            dma((SWEEPS, chunks, 2)),
            dma((SWEEPS, chunks, 2)),
            dma((SWEEPS, chunks, LINE)),
            dma((SWEEPS, chunks, LINE)),
            dma((SWEEPS, chunks, rows_n // LINE)),
            dma((SWEEPS, chunks, rows_n // LINE)),
            dma((rhs_n,)),
            dma((rhs_n,)),
        ],
        compiler_params=pltpu.CompilerParams(
            collective_id=0, has_side_effects=True, vmem_limit_bytes=54 * 1024 * 1024
        ),
        name="refine",
    )(band_blocks, precond_blocks, right_side)
    x, r, history, overall = pl.pallas_call(
        write_out,
        out_shape=(
            jax.ShapeDtypeStruct((n_rows, n_cols), F32),
            jax.ShapeDtypeStruct((n_rows, n_cols), F32),
            jax.ShapeDtypeStruct((SWEEPS, n_cols), F32),
            jax.ShapeDtypeStruct((1, 128), F32),
        ),
        in_specs=[pl.BlockSpec(memory_space=vmem)] * 4,
        out_specs=[pl.BlockSpec(memory_space=pltpu.HBM)] * 4,
        scratch_shapes=[dma((2, PIECES)), dma((2,))],
        compiler_params=pltpu.CompilerParams(vmem_limit_bytes=1024 * 1024),
        name="write_out",
    )(x, r, history, overall)
    return x, r, history, overall[0, 0]


def solution(mesh):
    rows_n, rhs_n = mesh.shape["rows"], mesh.shape["rhs"]
    in_specs = (P("rows", None, None), P("rows", None, None), P("rows", "rhs"))
    out_specs = (P("rows", "rhs"), P("rows", "rhs"), P(None, "rhs"), P())
    return jax.shard_map(
        functools.partial(shards, rows_n, rhs_n),
        mesh=mesh,
        in_specs=in_specs,
        out_specs=out_specs,
        check_vma=False,
    )
```

```python
import functools

import jax
import jax.numpy as jnp
from jax import lax
from jax.experimental import pallas as pl
from jax.experimental.pallas import tpu as pltpu
from jax.sharding import PartitionSpec as P

MESH = pl.DeviceIdType.MESH
F32, BF16 = jnp.float32, jnp.bfloat16
SWEEPS = 3
T = 256
PIECES = 4
LINE = 8


def split(value):
    high = value.astype(BF16)
    return high, (value - high.astype(F32)).astype(BF16)


def kernel(
    rows_n, rhs_n, blocks,
    band, precond, rhs,
    x, r, history, overall,
    a32, m32, ahi, alo, mhi, mlo, rhi, rlo, dhi, dlo, dsend, halo, hhi, hlo, part, msg, p1, mid, p2, zmsg, zbuf,
    ready, all_ready, last_msg, last_all, last_send, last_recv,
    a_sem, m_sem, b_sem, send_sem, recv_sem, p1_send, p1_recv, p2_send, p2_recv, z_send, z_recv,
):
    me = lax.axis_index("rows")
    z = lax.axis_index("rhs")
    lines = rows_n // LINE
    line, spot = me // LINE, me % LINE
    has = (me > 0, me < rows_n - 1)
    beside = (me - 1, me + 1)
    far = ((spot == 0) & has[0], (spot == LINE - 1) & has[1])
    chunks = rhs.shape[1] // T
    assert chunks == 2
    edge = (0, 1, blocks - 1, blocks - 2)
    inner = tuple(range(2, blocks // 2)), tuple(range(blocks - 3, blocks // 2 - 1, -1))
    inner_flat = tuple(j for pair in zip(*inner) for j in pair)

    def rows_of(j):
        return slice(j * T, (j + 1) * T)

    def cols_of(c):
        if isinstance(c, int):
            return slice(c * T, (c + 1) * T)
        return pl.ds(pl.multiple_of(c * T, T), T)

    def m_copy(j):
        return pltpu.make_async_copy(precond.at[j], m32.at[j], m_sem.at[j])

    def b_copy(j, c):
        return pltpu.make_async_copy(
            rhs.at[rows_of(j), cols_of(c)], r.at[rows_of(j), cols_of(c)], b_sem.at[j, c]
        )

    def a_copy(j):
        return pltpu.make_async_copy(band.at[j], a32.at[j], a_sem.at[j])

    for j in edge:
        m_copy(j).start()
    for c in range(chunks):
        for j in edge:
            b_copy(j, c).start(priority=min(c, 1))
    for j in inner_flat:
        m_copy(j).start(priority=1)
    for c in range(chunks):
        for j in inner_flat:
            b_copy(j, c).start(priority=1)
    band_pairs = tuple(zip((0, 1, *inner[0]), (blocks - 1, blocks - 2, *inner[1])))
    for pair in band_pairs:
        for j in pair:
            a_copy(j).start(priority=1)

    barrier = pltpu.get_barrier_semaphore()
    for k in range(1, LINE):
        pl.semaphore_signal(
            barrier, inc=1, device_id={"rows": line * LINE + (spot + k) % LINE}, device_id_type=MESH
        )
    for k in range(1, lines):
        pl.semaphore_signal(
            barrier, inc=1, device_id={"rows": (line + k) % lines * LINE + spot}, device_id_type=MESH
        )
    for k in range(1, rhs_n):
        pl.semaphore_signal(barrier, inc=1, device_id={"rhs": (z + k) % rhs_n}, device_id_type=MESH)
    for side in range(2):

        @pl.when(far[side])
        def _():
            pl.semaphore_signal(barrier, inc=1, device_id={"rows": beside[side]}, device_id_type=MESH)

    peers = LINE - 1 + lines - 1 + rhs_n - 1

    def body(*accs):
        acc = (accs[:2], accs[2:])
        turn = [0]

        def products(jobs):
            pick = turn[0] % 2
            turn[0] += 1
            for step in range(max(len(job) for job in jobs)):
                for unit in range(2):
                    if step < len(jobs[unit]):
                        pltpu.matmul_push_rhs(
                            jobs[unit][step][0][...], staging_register=step % 2, mxu_index=unit
                        )
                for unit in range(2):
                    if step < len(jobs[unit]):
                        staged = step % 2
                        for left in jobs[unit][step][1]:
                            pltpu.matmul_acc_lhs(acc[unit][pick], left[...], load_staged_rhs=staged)
                            staged = None
            return [pltpu.matmul_pop(acc[unit][pick]) for unit in range(2)]

        def terms(left_high, left_low, right_high, right_low):
            return [(right_high, (left_high, left_low)), (right_low, (left_high,))]

        def band_terms(i, k, right_high, right_low):
            cut = (i, slice(None), slice(k * T, (k + 1) * T))
            return terms(ahi.at[cut], alo.at[cut], right_high, right_low)

        def precondition(pairs, s, c, first):
            for pair in pairs:
                values = products(
                    [terms(mhi.at[j], mlo.at[j], rhi.at[c, j], rlo.at[c, j]) for j in pair]
                )
                for j, value in zip(pair, values):
                    where = (rows_of(j), cols_of(c))
                    if first:
                        x[where] = value
                    else:
                        x[where] = x[where] + value
                    dhi[c, j], dlo[c, j] = split(value)
                    if j < 2:
                        dsend[s, c, 0, j] = value
                    elif j >= blocks - 2:
                        dsend[s, c, 1, j - (blocks - 2)] = value

        def settle(s, c, j, value, keep):
            where = (rows_of(j), cols_of(c))
            value = r[where] - value
            r[where] = value
            if keep:
                rhi[c, j], rlo[c, j] = split(value)
            return value

        def squares(s, c, values):
            total = part[s, c]
            for value in values:
                total = total + jnp.sum((value * value).reshape(T // 8, 8, T), axis=0)
            part[s, c] = total

        def local(s, c, pairs):
            for pair in pairs:
                jobs = []
                for i in pair:
                    job = []
                    for k in range(5):
                        j = i + k - 2
                        if 0 <= j < blocks:
                            job += band_terms(i, k, dhi.at[c, j], dlo.at[c, j])
                    jobs.append(job)
                values = products(jobs)
                for i, value in zip(pair, values):
                    if i in edge:
                        where = (rows_of(i), cols_of(c))
                        r[where] = r[where] - value
                    else:
                        squares(s, c, [settle(s, c, i, value, True)])

        def halo_copy(s, c, side):
            return pltpu.make_async_remote_copy(
                src_ref=dsend.at[s, c, side],
                dst_ref=halo.at[s, c, 1 - side],
                send_sem=send_sem.at[s, c, side],
                recv_sem=recv_sem.at[s, c, 1 - side],
                device_id={"rows": beside[side]},
                device_id_type=MESH,
            )

        def send(s, c):
            for side in range(2):

                @pl.when(has[side])
                def _():
                    halo_copy(s, c, side).start()

        def sent(s, c):
            for side in range(2):

                @pl.when(has[side])
                def _():
                    halo_copy(s, c, side).wait_send()

        def arrive(s, c):
            for side in range(2):

                @pl.when(has[side])
                def _():
                    pltpu.make_async_remote_copy(
                        src_ref=dsend.at[s, c, side],
                        dst_ref=halo.at[s, c, side],
                        send_sem=send_sem.at[s, c, side],
                        recv_sem=recv_sem.at[s, c, side],
                        device_id={"rows": beside[side]},
                        device_id_type=MESH,
                    ).wait_recv()

        def remote(s, c, keep):
            for side in range(2):
                for q in range(2):
                    hhi[side, q], hlo[side, q] = split(halo[s, c, side, q])
            low = lambda q: (hhi.at[0, q], hlo.at[0, q])
            high = lambda q: (hhi.at[1, q], hlo.at[1, q])
            for pair, jobs in (
                (
                    (0, blocks - 1),
                    (
                        band_terms(0, 0, *low(0)) + band_terms(0, 1, *low(1)),
                        band_terms(blocks - 1, 3, *high(0)) + band_terms(blocks - 1, 4, *high(1)),
                    ),
                ),
                (
                    (1, blocks - 2),
                    (band_terms(1, 0, *low(1)), band_terms(blocks - 2, 4, *high(0))),
                ),
            ):
                values = products(jobs)
                squares(s, c, [settle(s, c, i, value, keep) for i, value in zip(pair, values)])

        def p1_copy(s, c, k):
            return pltpu.make_async_remote_copy(
                src_ref=msg.at[s, c],
                dst_ref=p1.at[s, c, k],
                send_sem=p1_send.at[s, c, k],
                recv_sem=p1_recv.at[s, c, k],
                device_id={"rows": line * LINE + (spot + k) % LINE},
                device_id_type=MESH,
            )

        def p2_copy(s, c, k):
            return pltpu.make_async_remote_copy(
                src_ref=mid.at[s, c],
                dst_ref=p2.at[s, c, k],
                send_sem=p2_send.at[s, c, k],
                recv_sem=p2_recv.at[s, c, k],
                device_id={"rows": (line + k) % lines * LINE + spot},
                device_id_type=MESH,
            )

        def sum_line(s, c):
            msg[s, c] = jnp.sum(part[s, c], axis=0, keepdims=True)
            for k in range(1, LINE):
                p1_copy(s, c, k).start()

        def sum_lines(s, c):
            total = msg[s, c]
            for k in range(1, LINE):
                p1_copy(s, c, k).wait()
                total = total + p1[s, c, k]
            mid[s, c] = total
            for k in range(1, lines):
                p2_copy(s, c, k).start()

        def summed(s, c):
            total = mid[s, c]
            for k in range(1, lines):
                p2_copy(s, c, k).wait()
                total = total + p2[s, c, k]
            return total

        def ready_rhs(js, c):
            for j in js:
                b_copy(j, c).wait()
                rhi[c, j], rlo[c, j] = split(r[rows_of(j), cols_of(c)])

        def ready_precond(js):
            for j in js:
                m_copy(j).wait()
                mhi[j], mlo[j] = split(m32[j])

        edge_pairs = ((0, blocks - 1), (1, blocks - 2))
        inner_pairs = tuple(zip(*inner))

        def ready_band(js):
            for j in js:
                a_copy(j).wait()
            for j in js:
                ahi[j], alo[j] = split(a32[j])

        ready_precond(edge)
        for c in range(chunks):
            ready_rhs(edge, c)
            precondition(edge_pairs, 0, c, True)
            if c == 0:
                pl.semaphore_wait(
                    barrier, peers + far[0].astype(jnp.int32) + far[1].astype(jnp.int32)
                )
            send(0, c)
        for k in range(1, LINE):
            pl.semaphore_signal(
                ready, inc=1, device_id={"rows": line * LINE + (spot + k) % LINE}, device_id_type=MESH
            )
        part[...] = jnp.zeros_like(part)
        for side in range(2):

            @pl.when(jnp.logical_not(has[side]))
            def _():
                halo[:, :, side] = jnp.zeros_like(halo[:, :, side])

        for j in inner_flat:
            m_copy(j).wait()
            for c in range(chunks):
                b_copy(j, c).wait()
        for j in inner_flat:
            mhi[j], mlo[j] = split(m32[j])
        for c in range(chunks):
            for j in inner_flat:
                rhi[c, j], rlo[c, j] = split(r[rows_of(j), cols_of(c)])
            precondition(inner_pairs, 0, c, True)
        ready_band(band_pairs[0])
        for n, pair in enumerate(band_pairs):
            if n + 1 < len(band_pairs):
                ready_band(band_pairs[n + 1])
            for c in range(chunks):
                if c == 0 or pair in edge_pairs:
                    local(0, c, (pair,))

        def unit(u, carry):
            s, c = u // chunks, u % chunks
            precondition(inner_pairs[:1], s + 1, c, False)
            arrive(s, c)
            remote(s, c, True)
            precondition(inner_pairs[1:], s + 1, c, False)
            precondition(edge_pairs, s + 1, c, False)
            sum_line(s, c)
            send(s + 1, c)
            local((u + 1) // chunks, 1 - c, inner_pairs[::-1])
            local(s + 1, c, edge_pairs[::-1])
            return carry

        lax.fori_loop(0, (SWEEPS - 1) * chunks, unit, 0)

        def last_copy(k):
            return pltpu.make_async_remote_copy(
                src_ref=last_msg,
                dst_ref=last_all.at[k],
                send_sem=last_send.at[k],
                recv_sem=last_recv.at[k],
                device_id={
                    "rows": (line + k // LINE) % lines * LINE + (spot + k % LINE) % LINE
                },
                device_id_type=MESH,
            )

        def z_copy(n):
            return pltpu.make_async_remote_copy(
                src_ref=zmsg,
                dst_ref=zbuf.at[n],
                send_sem=z_send.at[n],
                recv_sem=z_recv.at[n],
                device_id={
                    "rows": (line + n // rhs_n) % lines * LINE + spot,
                    "rhs": (z + n % rhs_n) % rhs_n,
                },
                device_id_type=MESH,
            )

        last = SWEEPS - 1
        earlier = [(s, c) for s in range(last) for c in range(chunks)]
        local(last, chunks - 1, inner_pairs)
        for c in range(chunks):
            arrive(last, c)
            remote(last, c, False)
            last_msg[:, cols_of(c)] = jnp.sum(part[last, c], axis=0, keepdims=True)
            if c == 0:
                pl.semaphore_wait(ready, LINE - 1)
                for k in range(1, rhs_n):
                    pl.semaphore_signal(
                        all_ready, inc=1, device_id={"rhs": (z + k) % rhs_n}, device_id_type=MESH
                    )
                for s, other in earlier:
                    sum_lines(s, other)
        for k in range(1, rows_n):
            last_copy(k).start()
        last_all[0] = last_msg[...]
        pl.semaphore_wait(all_ready, rhs_n - 1)
        for k in range(1, LINE):
            last_copy(k).wait()
        grand = jnp.sum(jnp.sum(last_all[:LINE], axis=0), axis=1, keepdims=True)
        zmsg[...] = jnp.broadcast_to(grand, zmsg.shape)
        for n in range(1, lines * rhs_n):
            z_copy(n).start()
        for s in range(SWEEPS):
            for c in range(chunks):
                sent(s, c)
        for s, c in earlier:
            history[s : s + 1, cols_of(c)] = jnp.sqrt(summed(s, c) / (rows_n * blocks * T) + 1e-06)
        for k in range(LINE, rows_n):
            last_copy(k).wait()
        total = jnp.sum(last_all[...], axis=0)
        root = jnp.sqrt(total / (rows_n * blocks * T) + 1e-06)
        history[last : last + 1] = root
        inverse = 1.0 / root
        for j in range(blocks):
            r[rows_of(j)] = r[rows_of(j)] * inverse
        grand = zmsg[...]
        for n in range(1, lines * rhs_n):
            z_copy(n).wait()
            grand = grand + zbuf[n]
        overall[...] = jnp.sqrt(grand / (rows_n * blocks * T * rhs_n * rhs.shape[1]) + 1e-06)

    pl.run_scoped(body, *([pltpu.ACC(0)((T, T), F32)] * 2), *([pltpu.ACC(1)((T, T), F32)] * 2))


def write_out(x, r, history, overall, x_out, r_out, history_out, overall_out, sem, small_sem):
    height = x.shape[0] // PIECES
    copies = [
        pltpu.make_async_copy(history, history_out, small_sem.at[0]),
        pltpu.make_async_copy(overall, overall_out, small_sem.at[1]),
    ]
    for n in range(PIECES):
        rows = slice(n * height, (n + 1) * height)
        copies.append(pltpu.make_async_copy(x.at[rows], x_out.at[rows], sem.at[0, n]))
        copies.append(pltpu.make_async_copy(r.at[rows], r_out.at[rows], sem.at[1, n]))
    for copy in copies:
        copy.start()
    for copy in copies:
        copy.wait()


def shards(rows_n, rhs_n, band_blocks, precond_blocks, right_side):
    blocks = band_blocks.shape[0]
    n_rows, n_cols = right_side.shape
    chunks = n_cols // T
    band_blocks, precond_blocks, right_side = (
        pltpu.with_memory_space_constraint(v, pltpu.HBM) for v in (band_blocks, precond_blocks, right_side)
    )
    dma = pltpu.SemaphoreType.DMA
    vmem = pltpu.VMEM
    x, r, history, overall = pl.pallas_call(
        functools.partial(kernel, rows_n, rhs_n, blocks),
        out_shape=(
            vmem((n_rows, n_cols), F32),
            vmem((n_rows, n_cols), F32),
            vmem((SWEEPS, n_cols), F32),
            vmem((1, 128), F32),
        ),
        in_specs=[pl.BlockSpec(memory_space=pltpu.HBM)] * 3,
        out_specs=[pl.BlockSpec(memory_space=vmem)] * 4,
        scratch_shapes=[
            vmem((blocks, T, 5 * T), F32),
            vmem((blocks, T, T), F32),
            vmem((blocks, T, 5 * T), BF16),
            vmem((blocks, T, 5 * T), BF16),
            vmem((blocks, T, T), BF16),
            vmem((blocks, T, T), BF16),
            vmem((chunks, blocks, T, T), BF16),
            vmem((chunks, blocks, T, T), BF16),
            vmem((chunks, blocks, T, T), BF16),
            vmem((chunks, blocks, T, T), BF16),
            vmem((SWEEPS, chunks, 2, 2, T, T), F32),
            vmem((SWEEPS, chunks, 2, 2, T, T), F32),
            vmem((2, 2, T, T), BF16),
            vmem((2, 2, T, T), BF16),
            vmem((SWEEPS, chunks, 8, T), F32),
            vmem((SWEEPS, chunks, 1, T), F32),
            vmem((SWEEPS, chunks, LINE, 1, T), F32),
            vmem((SWEEPS, chunks, 1, T), F32),
            vmem((SWEEPS, chunks, rows_n // LINE, 1, T), F32),
            vmem((1, 128), F32),
            vmem((rows_n // LINE * rhs_n, 1, 128), F32),
            pltpu.SemaphoreType.REGULAR,
            pltpu.SemaphoreType.REGULAR,
            vmem((1, n_cols), F32),
            vmem((rows_n, 1, n_cols), F32),
            dma((rows_n,)),
            dma((rows_n,)),
            dma((blocks,)),
            dma((blocks,)),
            dma((blocks, chunks)),
            dma((SWEEPS, chunks, 2)),
            dma((SWEEPS, chunks, 2)),
            dma((SWEEPS, chunks, LINE)),
            dma((SWEEPS, chunks, LINE)),
            dma((SWEEPS, chunks, rows_n // LINE)),
            dma((SWEEPS, chunks, rows_n // LINE)),
            dma((rows_n // LINE * rhs_n,)),
            dma((rows_n // LINE * rhs_n,)),
        ],
        compiler_params=pltpu.CompilerParams(
            collective_id=0, has_side_effects=True, vmem_limit_bytes=54 * 1024 * 1024
        ),
        name="refine",
    )(band_blocks, precond_blocks, right_side)
    x, r, history, overall = pl.pallas_call(
        write_out,
        out_shape=(
            jax.ShapeDtypeStruct((n_rows, n_cols), F32),
            jax.ShapeDtypeStruct((n_rows, n_cols), F32),
            jax.ShapeDtypeStruct((SWEEPS, n_cols), F32),
            jax.ShapeDtypeStruct((1, 128), F32),
        ),
        in_specs=[pl.BlockSpec(memory_space=vmem)] * 4,
        out_specs=[pl.BlockSpec(memory_space=pltpu.HBM)] * 4,
        scratch_shapes=[dma((2, PIECES)), dma((2,))],
        compiler_params=pltpu.CompilerParams(vmem_limit_bytes=1024 * 1024),
        name="write_out",
    )(x, r, history, overall)
    return x, r, history, overall[0, 0]


def solution(mesh):
    rows_n, rhs_n = mesh.shape["rows"], mesh.shape["rhs"]
    in_specs = (P("rows", None, None), P("rows", None, None), P("rows", "rhs"))
    out_specs = (P("rows", "rhs"), P("rows", "rhs"), P(None, "rhs"), P())
    return jax.shard_map(
        functools.partial(shards, rows_n, rhs_n),
        mesh=mesh,
        in_specs=in_specs,
        out_specs=out_specs,
        check_vma=False,
    )
```
